32 devices in a mesh: videos: 2 (over x), tokens: 4 (over z), frames: 4 (over y, core).
Axes of the slice: x: 2, y: 2, z: 4, core: 2. Of those that a mesh axis runs over, the one named last changes fastest.
Arguments:
- z_queue: float32 [128, 256, 4], P(('videos', 'frames'), 'tokens'), parts along dimension 0
- ada_mod: float32 [128, 3, 6, 1024], P(('videos', 'frames')), parts along dimension 0
- step_size: float32 [128], P(('videos', 'frames')), parts along dimension 0
- new_noise: float32 [4, 256, 4], P('videos', 'tokens'), parts along dimension 0
- lag_bias: float32 [3, 16, 16], replicated
- w_in: bfloat16 [4, 1024], replicated
- w_out: bfloat16 [1024, 4], replicated
- w_sqkv: bfloat16 [3, 1024, 3, 16, 64], replicated
- w_so: bfloat16 [3, 16, 64, 1024], replicated
- w_tqkv: bfloat16 [3, 1024, 3, 16, 64], replicated
- w_to: bfloat16 [3, 16, 64, 1024], replicated
- w_up: bfloat16 [3, 1024, 4096], replicated
- w_down: bfloat16 [3, 4096, 1024], replicated
Outputs:
- output 1: float32 [4, 256, 4], P('videos', ('tokens', 'frames')), parts along dimension 0
- output 2: float32 [128, 256, 4], P(('videos', 'frames'), 'tokens'), parts along dimension 0
There are 2 independent parts. The reference program is written for one: setup_inputs(seed, part) draws one part's arguments, and reference() takes and returns one part's arrays. A program takes and returns all parts, laid end to end along the dimension named above; an argument that names none is the same for every part.
All inputs are finite; a program needn't handle non-finite values.
Results may differ from the reference program's by a relative error of at most 0.00847983.
Values are sent between devices in bfloat16 or wider.
A program may use at most 1 GiB of HBM per device.

```python
import jax
import jax.numpy as jnp
from jax import lax

FRAMES = 64
PATCHES = 256
CHANNELS = 4
D = 1024
HEADS = 16
HEAD = 64
WINDOW = 16
LAYERS = 3
STEPS = 2


def setup_inputs(seed: int = 0, part: int = 0) -> dict:
    base_key = jax.random.key(seed)
    part_keys = jax.random.split(jax.random.fold_in(base_key, part), 4)
    shared_keys = jax.random.split(jax.random.fold_in(base_key, 100003), 9)
    z_queue = jax.random.normal(part_keys[0], (FRAMES, PATCHES, CHANNELS), jnp.float32)
    ada_mod = 0.4 * jax.random.normal(part_keys[1], (FRAMES, LAYERS, 6, D), jnp.float32)
    step_size = jax.random.uniform(part_keys[2], (FRAMES,), jnp.float32, 0.2, 0.6)
    new_noise = jax.random.normal(part_keys[3], (STEPS, PATCHES, CHANNELS), jnp.float32)
    lag_bias = jax.random.normal(shared_keys[0], (LAYERS, HEADS, WINDOW), jnp.float32)
    qkv_gain = jnp.array([2.0, 1.0, 1.0], jnp.float32)[:, None, None]
    w_in = (jax.random.normal(shared_keys[1], (CHANNELS, D), jnp.float32) * CHANNELS ** -0.5).astype(jnp.bfloat16)
    w_out = (jax.random.normal(shared_keys[2], (D, CHANNELS), jnp.float32) * D ** -0.5).astype(jnp.bfloat16)
    w_sqkv = (jax.random.normal(shared_keys[3], (LAYERS, D, 3, HEADS, HEAD), jnp.float32) * qkv_gain * D ** -0.5).astype(jnp.bfloat16)
    w_so = (jax.random.normal(shared_keys[4], (LAYERS, HEADS, HEAD, D), jnp.float32) * D ** -0.5).astype(jnp.bfloat16)
    w_tqkv = (jax.random.normal(shared_keys[5], (LAYERS, D, 3, HEADS, HEAD), jnp.float32) * D ** -0.5).astype(jnp.bfloat16)
    w_to = (jax.random.normal(shared_keys[6], (LAYERS, HEADS, HEAD, D), jnp.float32) * D ** -0.5).astype(jnp.bfloat16)
    w_up = (jax.random.normal(shared_keys[7], (LAYERS, D, 4 * D), jnp.float32) * D ** -0.5).astype(jnp.bfloat16)
    w_down = (jax.random.normal(shared_keys[8], (LAYERS, 4 * D, D), jnp.float32) * (4 * D) ** -0.5).astype(jnp.bfloat16)
    return dict(z_queue=z_queue, ada_mod=ada_mod, step_size=step_size, new_noise=new_noise, lag_bias=lag_bias, w_in=w_in, w_out=w_out, w_sqkv=w_sqkv, w_so=w_so, w_tqkv=w_tqkv, w_to=w_to, w_up=w_up, w_down=w_down)


def layer_norm(xres):
    row_mean = jnp.mean(xres, axis=-1, keepdims=True)
    centered = xres - row_mean
    row_var = jnp.mean(centered * centered, axis=-1, keepdims=True)
    return centered * lax.rsqrt(row_var + 1e-6)


def modulate(xres, mod_l, which):
    shift_vec = mod_l[..., None, 2 * which, :]
    scale_vec = mod_l[..., None, 2 * which + 1, :]
    return (layer_norm(xres) * (1.0 + scale_vec) + shift_vec).astype(jnp.bfloat16)


def spatial_attention(u_act, w_qkv, w_proj):
    qkv_all = jnp.dot(u_act.reshape(-1, D), w_qkv.reshape(D, 3 * D), preferred_element_type=jnp.float32).astype(jnp.bfloat16).reshape(FRAMES, PATCHES, 3, HEADS, HEAD)

    def frame_attention(frame_qkv):
        qkv_wide = frame_qkv.astype(jnp.float32)
        scores = jnp.einsum('qhe,khe->hqk', qkv_wide[:, 0], qkv_wide[:, 1]) * HEAD ** -0.5
        attn_prob = jax.nn.softmax(scores, axis=-1).astype(jnp.bfloat16).astype(jnp.float32)
        return jnp.einsum('hqk,khe->qhe', attn_prob, qkv_wide[:, 2]).astype(jnp.bfloat16)

    attn_out = lax.map(frame_attention, qkv_all)
    return jnp.dot(attn_out.reshape(-1, D), w_proj.reshape(D, D), preferred_element_type=jnp.float32).reshape(FRAMES, PATCHES, D)


def temporal_attention(u_act, w_qkv, w_proj, lag_bias):
    qkv_all = jnp.dot(u_act.reshape(-1, D), w_qkv.reshape(D, 3 * D), preferred_element_type=jnp.float32).astype(jnp.bfloat16).reshape(FRAMES, PATCHES, 3, HEADS, HEAD)
    by_token = jnp.swapaxes(qkv_all, 0, 1)
    offset_idx = jnp.arange(WINDOW)[:, None, None]
    frame_idx = jnp.arange(FRAMES)[None, :, None]
    bias_rows = jnp.transpose(lag_bias)[:, None, :]

    def token_attention(tok_qkv):
        qkv_wide = tok_qkv.astype(jnp.float32)
        keys_pad = jnp.pad(qkv_wide[:, 1], ((WINDOW - 1, 0), (0, 0), (0, 0)))
        vals_pad = jnp.pad(qkv_wide[:, 2], ((WINDOW - 1, 0), (0, 0), (0, 0)))
        scores = jnp.stack([jnp.sum(qkv_wide[:, 0] * keys_pad[WINDOW - 1 - offset:WINDOW - 1 - offset + FRAMES], axis=-1) for offset in range(WINDOW)], axis=0)
        scores = scores * HEAD ** -0.5 + bias_rows
        scores = jnp.where(frame_idx >= offset_idx, scores, -1e30)
        attn_prob = jax.nn.softmax(scores, axis=0).astype(jnp.bfloat16).astype(jnp.float32)
        mixed = sum(attn_prob[offset][:, :, None] * vals_pad[WINDOW - 1 - offset:WINDOW - 1 - offset + FRAMES] for offset in range(WINDOW))
        return mixed.astype(jnp.bfloat16)

    attn_out = jnp.swapaxes(lax.map(token_attention, by_token), 0, 1)
    return jnp.dot(attn_out.reshape(-1, D), w_proj.reshape(D, D), preferred_element_type=jnp.float32).reshape(FRAMES, PATCHES, D)


def mlp_block(u_act, w_up, w_down):
    hidden = jnp.dot(u_act.reshape(-1, D), w_up, preferred_element_type=jnp.float32)
    act_out = jax.nn.gelu(hidden, approximate=True).astype(jnp.bfloat16)
    return jnp.dot(act_out, w_down, preferred_element_type=jnp.float32).reshape(FRAMES, PATCHES, D)


def denoise(z_cur, ada_mod, step_size, lag_bias, w_in, w_out, w_sqkv, w_so, w_tqkv, w_to, w_up, w_down):
    xres = jnp.dot(z_cur.astype(jnp.bfloat16).reshape(-1, CHANNELS), w_in, preferred_element_type=jnp.float32).astype(jnp.bfloat16).astype(jnp.float32).reshape(FRAMES, PATCHES, D)

    def one_layer(xcur, layer_in):
        mod_l, bias_l, sqkv_l, so_l, tqkv_l, to_l, up_l, down_l = layer_in
        xcur = xcur + spatial_attention(modulate(xcur, mod_l, 0), sqkv_l, so_l)
        xcur = xcur + temporal_attention(modulate(xcur, mod_l, 1), tqkv_l, to_l, bias_l)
        xcur = xcur + mlp_block(modulate(xcur, mod_l, 2), up_l, down_l)
        return xcur, None

    xres = lax.scan(one_layer, xres, (jnp.swapaxes(ada_mod, 0, 1), lag_bias, w_sqkv, w_so, w_tqkv, w_to, w_up, w_down))[0]
    velocity = jnp.dot(layer_norm(xres).astype(jnp.bfloat16).reshape(-1, D), w_out, preferred_element_type=jnp.float32).reshape(FRAMES, PATCHES, CHANNELS)
    return z_cur + step_size[:, None, None] * velocity


def reference(z_queue, ada_mod, step_size, new_noise, lag_bias, w_in, w_out, w_sqkv, w_so, w_tqkv, w_to, w_up, w_down):
    def one_step(z_cur, noise_frame):
        z_new = denoise(z_cur, ada_mod, step_size, lag_bias, w_in, w_out, w_sqkv, w_so, w_tqkv, w_to, w_up, w_down)
        return jnp.concatenate([z_new[1:], noise_frame[None]], axis=0), z_new[0]

    z_final, emitted = lax.scan(one_step, z_queue, new_noise)
    return emitted, z_final
```

```python
import functools

import jax
import jax.numpy as jnp
from jax import lax
from jax.experimental import pallas as pl
from jax.experimental.pallas import tpu as pltpu
from jax.sharding import PartitionSpec as P


F32 = jnp.float32
BF16 = jnp.bfloat16
LOG2E = 1.4426950408889634
D = 1024
HID = 4096
TOK = 256
HALF = 128
OWN = 4
GRP = 16
VMEM_LIMIT = 66_000_000
NT = (((1,), (1,)), ((), ()))
TN = (((0,), (0,)), ((), ()))
PART = 2


def dot(a, b):
    return jnp.dot(a, b, preferred_element_type=F32)


def dot_nt(a, b):
    return lax.dot_general(a, b, NT, preferred_element_type=F32)


def norm_rows(xb):
    mean = jnp.mean(xb, axis=-1, keepdims=True)
    cen = xb - mean
    var = jnp.mean(cen * cen, axis=-1, keepdims=True)
    return cen * lax.rsqrt(var + 1e-6)


def norm_mod(src, src_row, dst, dst_row, shift, scale, rows, blk=32):
    gain = 1.0 + scale

    def body(i, carry):
        rs = pl.multiple_of(src_row + i * blk, blk)
        rd = pl.multiple_of(dst_row + i * blk, blk)
        dst[pl.ds(rd, blk), :] = (norm_rows(src[pl.ds(rs, blk), :]) * gain + shift).astype(BF16)
        return carry

    lax.fori_loop(0, rows // blk, body, 0)


def gelu(v):
    return v * (0.5 + 0.5 * jnp.tanh(v * (0.7978845608028654 + (0.7978845608028654 * 0.044715) * (v * v))))


def dot_tn(a, b):
    return lax.dot_general(a, b, TN, preferred_element_type=F32)


def softmax_bf16(t):
    top = jnp.max(t, axis=0, keepdims=True)
    e = jnp.exp2(t - top)
    return (e * (1.0 / jnp.sum(e, axis=0, keepdims=True))).astype(BF16)


def half_masks():
    lane = lax.broadcasted_iota(jnp.int32, (1, 128), 1)
    low = (lane < 64).astype(F32)
    return low.astype(BF16), (1.0 - low).astype(BF16), lane < 64


def dense_kernel(*refs, do_c, do_a, ns, layer, part):
    it = iter(refs)
    x_in = next(it)
    if do_c:
        o_keep, o_recv, mod_c, wto, wup, wdn = (next(it) for _ in range(6))
    if do_a:
        mod_a, wsqkv, wso = (next(it) for _ in range(3))
    x = next(it)
    if do_a:
        u_keep, u_send = next(it), next(it)
    u_buf, o_buf = next(it), next(it)
    if do_c:
        vto, vup, vdn, h_buf = (next(it) for _ in range(4))
    if do_a:
        vsqkv, vso, qkv_buf = (next(it) for _ in range(3))
    sems = next(it)

    rows = ns * TOK
    core = lax.rem(lax.axis_index('frames'), 2)
    copies = []
    if do_c:
        copies += [pltpu.make_async_copy(wto.at[layer], vto, sems.at[0]),
                   pltpu.make_async_copy(wup.at[layer], vup, sems.at[1]),
                   pltpu.make_async_copy(wdn.at[layer], vdn, sems.at[2])]
    nxt = layer + 1 if do_c else layer
    if do_a:
        copies += [pltpu.make_async_copy(wsqkv.at[nxt], vsqkv, sems.at[3]),
                   pltpu.make_async_copy(wso.at[nxt], vso, sems.at[4])]
    state = {'next': 0}

    def start_more():
        if state['next'] < len(copies):
            copies[state['next']].start()
            state['next'] += 1

    def arrive(k):
        copies[k].wait()
        start_more()

    start_more()
    start_more()
    k = 0
    if do_c:
        for s in range(ns):
            o_buf[pl.ds(pl.multiple_of(s * TOK + core * HALF, HALF), HALF), :] = o_keep[part * ns + s]
            o_buf[pl.ds(pl.multiple_of(s * TOK + (1 - core) * HALF, HALF), HALF), :] = o_recv[part * ns + s]
        arrive(0)

        def proj(j, carry):
            c = pl.ds(pl.multiple_of(j * 256, 256), 256)
            x[:, c] = x_in[:, c] + dot(o_buf[...], vto[:, c])
            return carry

        lax.fori_loop(0, D // 256, proj, 0)
        for s in range(ns):
            norm_mod(x, s * TOK, u_buf, s * TOK, mod_c[s, 4:5, :], mod_c[s, 5:6, :], TOK)
        arrive(1)
        hrows = min(rows, 512)
        for b in range(rows // hrows):
            rb = pl.ds(b * hrows, hrows)

            def up(j, carry):
                c = pl.ds(pl.multiple_of(j * 256, 256), 256)
                h_buf[:, c] = gelu(dot(u_buf[rb, :], vup[:, c])).astype(BF16)
                return carry

            lax.fori_loop(0, HID // 256, up, 0)
            if b == 0:
                arrive(2)

            def down(j, carry):
                c = pl.ds(pl.multiple_of(j * 256, 256), 256)
                x[rb, c] = x[rb, c] + dot(h_buf[...], vdn[:, c])
                return carry

            lax.fori_loop(0, D // 256, down, 0)
        k = 3
    else:
        x[...] = x_in[...]
    if do_a:
        for s in range(ns):
            norm_mod(x, s * TOK, u_buf, s * TOK, mod_a[s, 0:1, :], mod_a[s, 1:2, :], TOK)
        arrive(k)

        def qkv(j, carry):
            c = pl.ds(pl.multiple_of(j * 256, 256), 256)
            qkv_buf[:, c] = dot_nt(u_buf[...], vsqkv[c, :]).astype(BF16)
            return carry

        lax.fori_loop(0, 3 * D // 256, qkv, 0)
        low, high, is_low = half_masks()

        def attend(i, carry):
            r = pl.ds(pl.multiple_of((i // 2) * TOK, TOK), TOK)
            for h in range(4):
                c = (i % 2) * 512 + h * 128
                q = qkv_buf[r, pl.ds(pl.multiple_of(c, 128), 128)]
                key = qkv_buf[r, pl.ds(pl.multiple_of(D + c, 128), 128)]
                val = qkv_buf[r, pl.ds(pl.multiple_of(2 * D + c, 128), 128)]
                both = jnp.concatenate([q * low, q * high], axis=0)
                mixed = dot_tn(softmax_bf16(dot_nt(key, both) * (0.125 * LOG2E)), val)
                o_buf[r, pl.ds(pl.multiple_of(c, 128), 128)] = jnp.where(is_low, mixed[:TOK], mixed[TOK:]).astype(BF16)
            return carry

        lax.fori_loop(0, ns * 2, attend, 0)
        arrive(k + 1)

        def proj_s(j, carry):
            c = pl.ds(pl.multiple_of(j * 256, 256), 256)
            x[:, c] = x[:, c] + dot(o_buf[...], vso[:, c])
            return carry

        lax.fori_loop(0, D // 256, proj_s, 0)
        for s in range(ns):
            norm_mod(x, s * TOK + core * HALF, u_keep.at[s], 0, mod_a[s, 2:3, :], mod_a[s, 3:4, :], HALF)
            norm_mod(x, s * TOK + (1 - core) * HALF, u_send.at[s], 0, mod_a[s, 2:3, :], mod_a[s, 3:4, :], HALF)


VM = pl.BlockSpec(memory_space=pltpu.VMEM)
HB = pl.BlockSpec(memory_space=pl.ANY)


def dense_call(layer, part, do_c, do_a, x, c_args, a_args):
    rows = x.shape[0]
    ns = rows // TOK
    args, specs = [x], [VM]
    if do_c:
        args += c_args
        specs += [VM, VM, VM, HB, HB, HB]
    if do_a:
        args += a_args
        specs += [VM, HB, HB]
    outs = [jax.ShapeDtypeStruct((rows, D), F32)]
    if do_a:
        outs += [jax.ShapeDtypeStruct((ns, HALF, D), BF16)] * 2
    scratch = [pltpu.VMEM((rows, D), BF16), pltpu.VMEM((rows, D), BF16)]
    if do_c:
        scratch += [pltpu.VMEM((D, D), BF16), pltpu.VMEM((D, HID), BF16), pltpu.VMEM((HID, D), BF16),
                    pltpu.VMEM((min(rows, 512), HID), BF16)]
    if do_a:
        scratch += [pltpu.VMEM((3 * D, D), BF16), pltpu.VMEM((D, D), BF16), pltpu.VMEM((rows, 3 * D), BF16)]
    scratch.append(pltpu.SemaphoreType.DMA((5,)))
    flops = 2 * rows * D * ((D + 2 * HID) * do_c + 4 * D * do_a)
    return pl.pallas_call(
        functools.partial(dense_kernel, do_c=do_c, do_a=do_a, ns=ns, layer=layer, part=part),
        out_shape=outs,
        in_specs=specs,
        out_specs=[VM] * len(outs),
        scratch_shapes=scratch,
        compiler_params=pltpu.CompilerParams(vmem_limit_bytes=VMEM_LIMIT),
        cost_estimate=pl.CostEstimate(flops=flops, bytes_accessed=rows * D * 8, transcendentals=0),
        name='dense',
    )(*args)


def own_kernel(*refs, layer):
    keeps, swaps = refs[:OWN // PART], refs[OWN // PART:2 * OWN // PART]
    wqkv, q, kv, u_buf, w_buf, sem = refs[2 * OWN // PART:]
    core = lax.rem(lax.axis_index('frames'), 2)
    copy = pltpu.make_async_copy(wqkv.at[layer], w_buf, sem)
    copy.start()
    for s in range(OWN):
        u_buf[pl.ds(pl.multiple_of((core * OWN + s) * HALF, HALF), HALF), :] = keeps[s // PART][s % PART]
        u_buf[pl.ds(pl.multiple_of(((1 - core) * OWN + s) * HALF, HALF), HALF), :] = swaps[s // PART][s % PART]
    copy.wait()

    def q_part(j, carry):
        c = pl.ds(pl.multiple_of(j * 256, 256), 256)
        q[:, :, c] = dot_nt(u_buf[...], w_buf[c, :]).astype(BF16).reshape(2 * OWN, HALF, 256)
        return carry

    lax.fori_loop(0, D // 256, q_part, 0)

    def kv_part(j, carry):
        c = pl.ds(pl.multiple_of(j * 256, 256), 256)
        w = w_buf[pl.ds(pl.multiple_of(D + j * 256, 256), 256), :]
        kv[:, :, c] = dot_nt(u_buf[...], w).astype(BF16).reshape(2 * OWN, HALF, 256)
        return carry

    lax.fori_loop(0, 2 * D // 256, kv_part, 0)


def own_call(layer, keeps, swaps, w_tqkv):
    rows = 2 * OWN * HALF
    return pl.pallas_call(
        functools.partial(own_kernel, layer=layer),
        out_shape=[jax.ShapeDtypeStruct((2 * OWN, HALF, D), BF16), jax.ShapeDtypeStruct((2 * OWN, HALF, 2 * D), BF16)],
        in_specs=[VM] * (2 * OWN // PART) + [HB],
        out_specs=[VM, VM],
        scratch_shapes=[pltpu.VMEM((rows, D), BF16), pltpu.VMEM((3 * D, D), BF16), pltpu.SemaphoreType.DMA],
        compiler_params=pltpu.CompilerParams(vmem_limit_bytes=VMEM_LIMIT),
        cost_estimate=pl.CostEstimate(flops=6 * rows * D * D, bytes_accessed=16 << 20, transcendentals=0),
        name='temporal_own',
    )(*keeps, *swaps, w_tqkv)


def halo_kernel(*refs, layer):
    n = OWN // PART
    q, kv_own = refs[:2]
    near_k, near_s, up_k, up_s, down_k, down_s = (refs[2 + n * i:2 + n * i + n] for i in range(6))
    bias_all, wqkv, o_keep, o_send, u_buf, kv, bias, w_buf, o_buf, sems, halo_sems = refs[2 + 6 * n:]
    pos = lax.axis_index('frames')
    core = lax.rem(pos, 2)
    other = 1 - core
    row = pos // 2
    cw = pltpu.make_async_copy(wqkv.at[layer, pl.ds(D, 2 * D)], w_buf, sems.at[0])
    cw.start()

    def into(src, slot, k):
        return [pltpu.make_async_copy(src[i], u_buf.at[pl.ds(slot + PART * i, PART)], halo_sems.at[k, i]) for i in range(n)]

    near = into(near_k, core * OWN, 0) + into(near_s, other * OWN, 1)
    up = into(up_k, (2 + core) * OWN, 2) + into(up_s, (2 + other) * OWN, 3)
    down = into(down_k, (2 + core) * OWN, 2) + into(down_s, (2 + other) * OWN, 3)
    for c in near:
        c.start()

    @pl.when(row == 1)
    def _():
        for c in up:
            c.start()

    @pl.when(row == 0)
    def _():
        for c in down:
            c.start()

    c4 = pltpu.make_async_copy(kv_own, kv.at[pl.ds(4 * OWN, 2 * OWN)], sems.at[1])
    c4.start()
    c5 = pltpu.make_async_copy(bias_all.at[layer], bias, sems.at[2])
    c5.start()
    for c in [cw] + near + up:
        c.wait()

    def fill(i, carry):
        s = (i // 8) * 4
        j = i % 8
        c = pl.ds(pl.multiple_of(j * 256, 256), 256)
        a = u_buf[pl.ds(s, 4)].reshape(4 * HALF, D)
        kv[pl.ds(s, 4), :, c] = dot_nt(a, w_buf[c, :]).astype(BF16).reshape(4, HALF, 256)
        return carry

    lax.fori_loop(0, 32, fill, 0)
    c4.wait()
    c5.wait()
    low, high, is_low = half_masks()

    def attend(i, carry):
        tok = pl.ds(pl.multiple_of(i * GRP, GRP), GRP)
        for hp in range(8):
            c = slice(hp * 128, hp * 128 + 128)
            qb = q[:, tok, c].reshape(2 * OWN * GRP, 128)
            key = kv[:, tok, c].reshape(6 * OWN * GRP, 128)
            val = kv[:, tok, D + hp * 128:D + hp * 128 + 128].reshape(6 * OWN * GRP, 128)
            mixed = []
            for e, m in enumerate((low, high)):
                t = dot_nt(key, qb * m) * (0.125 * LOG2E) + bias[2 * hp + e]
                mixed.append(dot_tn(softmax_bf16(t), val))
            o = jnp.where(is_low, mixed[0], mixed[1]).astype(BF16)
            o_buf[:, tok, c] = o.reshape(2 * OWN, GRP, 128)
        return carry

    lax.fori_loop(0, HALF // GRP, attend, 0)
    o_keep[...] = o_buf[pl.ds(core * OWN, OWN)]
    o_send[...] = o_buf[pl.ds(other * OWN, OWN)]


def halo_call(layer, q, kv_own, halos, bias, w_tqkv):
    n = 2 * OWN
    return pl.pallas_call(
        functools.partial(halo_kernel, layer=layer),
        out_shape=[jax.ShapeDtypeStruct((OWN, HALF, D), BF16)] * 2,
        in_specs=[VM] + [HB] * (3 + len(halos)),
        out_specs=[VM, VM],
        scratch_shapes=[pltpu.VMEM((2 * n, HALF, D), BF16), pltpu.VMEM((3 * n, HALF, 2 * D), BF16),
                        pltpu.VMEM((16, 3 * n * GRP, n * GRP), F32), pltpu.VMEM((2 * D, D), BF16),
                        pltpu.VMEM((n, HALF, D), BF16), pltpu.SemaphoreType.DMA((3,)),
                        pltpu.SemaphoreType.DMA((4, OWN // PART))],
        compiler_params=pltpu.CompilerParams(vmem_limit_bytes=VMEM_LIMIT),
        cost_estimate=pl.CostEstimate(flops=16 * n * HALF * D * D, bytes_accessed=16 << 20, transcendentals=0),
        name='temporal_halo',
    )(q, kv_own, *halos, bias, w_tqkv)


def bias_kernel(lag, out):
    base = 16 * (16 * lax.axis_index('tokens') + 8 * (lax.axis_index('frames') // 2))
    shape = out.shape[2:]
    col = lax.broadcasted_iota(jnp.int32, shape, 0)
    row = lax.broadcasted_iota(jnp.int32, shape, 1)
    gap = jnp.where(col + base >= 256, row + 256 - col, -1)
    layer = pl.program_id(0)

    def head(h, carry):
        acc = jnp.full(shape, -1e30, F32)
        for r in range(16):
            acc = jnp.where(gap == GRP * r, lag[layer, h, r] * LOG2E, acc)
        out[0, h] = acc
        return carry

    lax.fori_loop(0, 16, head, 0)


def bias_call(lag_bias):
    shape = (3, 16, 6 * OWN * GRP, 2 * OWN * GRP)
    return pl.pallas_call(
        bias_kernel,
        grid=(3,),
        out_shape=jax.ShapeDtypeStruct(shape, F32),
        in_specs=[pl.BlockSpec(memory_space=pltpu.SMEM)],
        out_specs=pl.BlockSpec((1,) + shape[1:], lambda i: (i, 0, 0, 0)),
        name='bias_table',
    )(lag_bias)


def solution(mesh):
    nz = mesh.shape['tokens']
    slot_spec = P(('videos', 'frames'), 'tokens', None)
    mod_spec = P(('videos', 'frames'), None, None, None)
    step_spec = P(('videos', 'frames'))
    noise_spec = P('videos', 'tokens', None)
    emit_spec = P('videos', ('tokens', 'frames'), None)
    group = ('tokens', 'frames')
    same = [(z * 4 + f, (z + 1) * 4 + f) for z in range(nz - 1) for f in range(4)]
    cross = [(z * 4 + f, (z + 1) * 4 + (f ^ 1)) for z in range(nz - 1) for f in range(4)]

    def body(z_loc, mod_loc, step_loc, noise_loc, lag_bias, w_in, w_out, w_sqkv, w_so, w_tqkv, w_to, w_up, w_down):
        zc = lax.axis_index('tokens')
        fc = lax.axis_index('frames')
        layers = w_up.shape[0]
        n_steps = noise_loc.shape[0]
        sq = jnp.transpose(w_sqkv, (0, 2, 3, 4, 1)).reshape(layers, 3 * D, D)
        tq = jnp.transpose(w_tqkv, (0, 2, 3, 4, 1)).reshape(layers, 3 * D, D)
        so = w_so.reshape(layers, D, D)
        to = w_to.reshape(layers, D, D)
        bias = bias_call(lag_bias)

        small = jnp.concatenate([z_loc.reshape(16, 256), noise_loc.reshape(n_steps, 256),
                                 jnp.pad(step_loc, (0, 240))[None]], axis=0)
        small = lax.all_gather(small, group, axis=0).reshape(nz, 4, 17 + n_steps, 256)
        z_all = small[:, :, :16].reshape(nz, 4, 16, 64, 4).transpose(1, 2, 0, 3, 4).reshape(64, TOK * 4)
        noise = small[:, 0, 16:16 + n_steps].reshape(nz, n_steps, 256).transpose(1, 0, 2).reshape(n_steps, TOK * 4)
        first = 16 * zc + 4 * fc
        dt = lax.dynamic_slice(small[0, :, 16 + n_steps, :16].reshape(64), (first,), (4,))
        mod = lax.all_to_all(mod_loc.reshape(4, 4, layers, 6, D), 'frames', 0, 0)
        mod = lax.dynamic_index_in_dim(mod, zc, 0, keepdims=False)
        mods = [[mod[p * PART:(p + 1) * PART, l] for p in range(OWN // PART)] for l in range(layers)]

        def one_step(s, z_all):
            z_cur = lax.dynamic_slice(z_all, (first, 0), (4, TOK * 4)).reshape(4 * TOK, 4)
            x = dot(z_cur.astype(BF16), w_in).astype(BF16).astype(F32)
            parts = range(OWN // PART)
            rows = PART * TOK
            xs = [x[p * rows:(p + 1) * rows] for p in parts]
            c_args = None
            for l in range(layers):
                keeps, sends = [], []
                for p in parts:
                    ca = () if c_args is None else c_args + [mods[l - 1][p], to, w_up, w_down]
                    xs[p], keep, send = dense_call(l - 1 if l else 0, p, l > 0, True, xs[p], ca, [mods[l][p], sq, so])
                    keeps.append(keep)
                    sends.append(send)

                def move(vals, axes, pairs):
                    out = []
                    for p in parts:
                        out.append(lax.ppermute(vals[p], axes, pairs))
                    return out

                near_k = move(keeps, group, same)
                near_s = move(sends, group, cross)
                up_k = move(keeps, 'frames', [(0, 2), (1, 3)])
                up_s = move(sends, 'frames', [(0, 3), (1, 2)])
                swaps = move(sends, 'frames', [(0, 1), (1, 0), (2, 3), (3, 2)])
                down_k = move(near_k, 'frames', [(2, 0), (3, 1)])
                down_s = move(near_s, 'frames', [(2, 0), (3, 1)])
                q, kv_own = own_call(l, keeps, swaps, tq)
                halos = near_k + near_s + up_k + up_s + down_k + down_s
                o_keep, o_send = halo_call(l, q, kv_own, halos, bias, tq)
                o_recv = lax.ppermute(o_send, 'frames', [(0, 1), (1, 0), (2, 3), (3, 2)])
                c_args = [o_keep, o_recv]
            xs = [dense_call(layers - 1, p, True, False, xs[p], c_args + [mods[layers - 1][p], to, w_up, w_down], ())[0]
                  for p in parts]
            x = jnp.concatenate(xs, axis=0)
            vel = dot(norm_rows(x).astype(BF16), w_out)
            z_new = (z_cur + jnp.repeat(dt, TOK)[:, None] * vel).reshape(4, TOK * 4)
            z_new = lax.all_gather(z_new, group, axis=0, tiled=True)
            emit = lax.dynamic_slice(z_new[0].reshape(TOK, 4), (64 * zc + 16 * fc, 0), (16, 4))
            return jnp.concatenate([z_new[1:], noise[s][None]], axis=0), emit

        emits = []
        for s in range(n_steps):
            z_all, emit = one_step(s, z_all)
            emits.append(emit)
        z_out = lax.dynamic_slice(z_all.reshape(64, TOK, 4), (16 * fc, 64 * zc, 0), (16, 64, 4))
        return jnp.stack(emits), z_out

    return jax.shard_map(body, mesh=mesh, in_specs=(slot_spec, mod_spec, step_spec, noise_spec) + (P(),) * 9,
                         out_specs=(emit_spec, slot_spec), check_vma=False)
```

```python
import functools

import jax
import jax.numpy as jnp
from jax import lax
from jax.experimental import pallas as pl
from jax.experimental.pallas import tpu as pltpu
from jax.sharding import PartitionSpec as P


F32 = jnp.float32
BF16 = jnp.bfloat16
LOG2E = 1.4426950408889634
D = 1024
HID = 4096
TOK = 256
HALF = 128
OWN = 4
GRP = 16
VMEM_LIMIT = 66_000_000
NT = (((1,), (1,)), ((), ()))
TN = (((0,), (0,)), ((), ()))
PART = 2


def dot(a, b):
    return jnp.dot(a, b, preferred_element_type=F32)


def dot_nt(a, b):
    return lax.dot_general(a, b, NT, preferred_element_type=F32)


def norm_rows(xb):
    mean = jnp.mean(xb, axis=-1, keepdims=True)
    cen = xb - mean
    var = jnp.mean(cen * cen, axis=-1, keepdims=True)
    return cen * lax.rsqrt(var + 1e-6)


def norm_mod(src, src_row, dst, dst_row, shift, scale, rows, blk=128):
    gain = 1.0 + scale

    def body(i, carry):
        rs = pl.multiple_of(src_row + i * blk, blk)
        rd = pl.multiple_of(dst_row + i * blk, blk)
        dst[pl.ds(rd, blk), :] = (norm_rows(src[pl.ds(rs, blk), :]) * gain + shift).astype(BF16)
        return carry

    lax.fori_loop(0, rows // blk, body, 0)


def gelu(v):
    return v * (0.5 + 0.5 * jnp.tanh(v * (0.7978845608028654 + (0.7978845608028654 * 0.044715) * (v * v))))


def dot_tn(a, b):
    return lax.dot_general(a, b, TN, preferred_element_type=F32)


def softmax_bf16(t):
    top = jnp.max(t, axis=0, keepdims=True)
    e = jnp.exp2(t - top)
    return (e * (1.0 / jnp.sum(e, axis=0, keepdims=True))).astype(BF16)


def half_masks():
    lane = lax.broadcasted_iota(jnp.int32, (1, 128), 1)
    low = (lane < 64).astype(F32)
    return low.astype(BF16), (1.0 - low).astype(BF16), lane < 64


def dense_kernel(*refs, do_c, do_a, ns, layer, part):
    it = iter(refs)
    x_in = next(it)
    if do_c:
        o_keep, o_recv, mod_c, wto, wup, wdn = (next(it) for _ in range(6))
    if do_a:
        mod_a, wsqkv, wso = (next(it) for _ in range(3))
    x = next(it)
    if do_a:
        u_keep, u_send = next(it), next(it)
    u_buf, o_buf = next(it), next(it)
    if do_c:
        vto, vup, vdn, h_buf = (next(it) for _ in range(4))
    if do_a:
        vsqkv, vso, qkv_buf = (next(it) for _ in range(3))
    sems = next(it)

    rows = ns * TOK
    core = lax.rem(lax.axis_index('frames'), 2)
    copies = []
    if do_c:
        copies += [pltpu.make_async_copy(wto.at[layer], vto, sems.at[0]),
                   pltpu.make_async_copy(wup.at[layer], vup, sems.at[1]),
                   pltpu.make_async_copy(wdn.at[layer], vdn, sems.at[2])]
    nxt = layer + 1 if do_c else layer
    if do_a:
        copies += [pltpu.make_async_copy(wsqkv.at[nxt], vsqkv, sems.at[3]),
                   pltpu.make_async_copy(wso.at[nxt], vso, sems.at[4])]
    state = {'next': 0}

    def start_more():
        if state['next'] < len(copies):
            copies[state['next']].start()
            state['next'] += 1

    def arrive(k):
        copies[k].wait()
        start_more()

    start_more()
    start_more()
    k = 0
    if do_c:
        for s in range(ns):
            o_buf[pl.ds(pl.multiple_of(s * TOK + core * HALF, HALF), HALF), :] = o_keep[part * ns + s]
            o_buf[pl.ds(pl.multiple_of(s * TOK + (1 - core) * HALF, HALF), HALF), :] = o_recv[part * ns + s]
        arrive(0)

        def proj(j, carry):
            c = pl.ds(pl.multiple_of(j * 256, 256), 256)
            x[:, c] = x_in[:, c] + dot(o_buf[...], vto[:, c])
            return carry

        lax.fori_loop(0, D // 256, proj, 0)
        for s in range(ns):
            norm_mod(x, s * TOK, u_buf, s * TOK, mod_c[s, 4:5, :], mod_c[s, 5:6, :], TOK)
        arrive(1)
        hrows = min(rows, 512)
        for b in range(rows // hrows):
            rb = pl.ds(b * hrows, hrows)

            def up(j, carry):
                c = pl.ds(pl.multiple_of(j * 256, 256), 256)
                h_buf[:, c] = gelu(dot(u_buf[rb, :], vup[:, c])).astype(BF16)
                return carry

            lax.fori_loop(0, HID // 256, up, 0)
            if b == 0:
                arrive(2)

            def down(j, carry):
                c = pl.ds(pl.multiple_of(j * 256, 256), 256)
                x[rb, c] = x[rb, c] + dot(h_buf[...], vdn[:, c])
                return carry

            lax.fori_loop(0, D // 256, down, 0)
        k = 3
    else:
        x[...] = x_in[...]
    if do_a:
        for s in range(ns):
            norm_mod(x, s * TOK, u_buf, s * TOK, mod_a[s, 0:1, :], mod_a[s, 1:2, :], TOK)
        arrive(k)

        def qkv(j, carry):
            c = pl.ds(pl.multiple_of(j * 256, 256), 256)
            qkv_buf[:, c] = dot_nt(u_buf[...], vsqkv[c, :]).astype(BF16)
            return carry

        lax.fori_loop(0, 3 * D // 256, qkv, 0)
        low, high, is_low = half_masks()

        def attend(i, carry):
            r = pl.ds(pl.multiple_of((i // 2) * TOK, TOK), TOK)
            for h in range(4):
                c = (i % 2) * 512 + h * 128
                q = qkv_buf[r, pl.ds(pl.multiple_of(c, 128), 128)]
                key = qkv_buf[r, pl.ds(pl.multiple_of(D + c, 128), 128)]
                val = qkv_buf[r, pl.ds(pl.multiple_of(2 * D + c, 128), 128)]
                both = jnp.concatenate([q * low, q * high], axis=0)
                mixed = dot_tn(softmax_bf16(dot_nt(key, both) * (0.125 * LOG2E)), val)
                o_buf[r, pl.ds(pl.multiple_of(c, 128), 128)] = jnp.where(is_low, mixed[:TOK], mixed[TOK:]).astype(BF16)
            return carry

        lax.fori_loop(0, ns * 2, attend, 0)
        arrive(k + 1)

        def proj_s(j, carry):
            c = pl.ds(pl.multiple_of(j * 256, 256), 256)
            x[:, c] = x[:, c] + dot(o_buf[...], vso[:, c])
            return carry

        lax.fori_loop(0, D // 256, proj_s, 0)
        for s in range(ns):
            norm_mod(x, s * TOK + core * HALF, u_keep.at[s], 0, mod_a[s, 2:3, :], mod_a[s, 3:4, :], HALF)
            norm_mod(x, s * TOK + (1 - core) * HALF, u_send.at[s], 0, mod_a[s, 2:3, :], mod_a[s, 3:4, :], HALF)


VM = pl.BlockSpec(memory_space=pltpu.VMEM)
HB = pl.BlockSpec(memory_space=pl.ANY)


def dense_call(layer, part, do_c, do_a, x, c_args, a_args):
    rows = x.shape[0]
    ns = rows // TOK
    args, specs = [x], [VM]
    if do_c:
        args += c_args
        specs += [VM, VM, VM, HB, HB, HB]
    if do_a:
        args += a_args
        specs += [VM, HB, HB]
    outs = [jax.ShapeDtypeStruct((rows, D), F32)]
    if do_a:
        outs += [jax.ShapeDtypeStruct((ns, HALF, D), BF16)] * 2
    scratch = [pltpu.VMEM((rows, D), BF16), pltpu.VMEM((rows, D), BF16)]
    if do_c:
        scratch += [pltpu.VMEM((D, D), BF16), pltpu.VMEM((D, HID), BF16), pltpu.VMEM((HID, D), BF16),
                    pltpu.VMEM((min(rows, 512), HID), BF16)]
    if do_a:
        scratch += [pltpu.VMEM((3 * D, D), BF16), pltpu.VMEM((D, D), BF16), pltpu.VMEM((rows, 3 * D), BF16)]
    scratch.append(pltpu.SemaphoreType.DMA((5,)))
    flops = 2 * rows * D * ((D + 2 * HID) * do_c + 4 * D * do_a)
    return pl.pallas_call(
        functools.partial(dense_kernel, do_c=do_c, do_a=do_a, ns=ns, layer=layer, part=part),
        out_shape=outs,
        in_specs=specs,
        out_specs=[VM] * len(outs),
        scratch_shapes=scratch,
        compiler_params=pltpu.CompilerParams(vmem_limit_bytes=VMEM_LIMIT),
        cost_estimate=pl.CostEstimate(flops=flops, bytes_accessed=rows * D * 8, transcendentals=0),
        name='dense',
    )(*args)


def project_kernel(*refs, layer, start, cols):
    n = OWN // PART
    mine, theirs = refs[:n], refs[n:2 * n]
    wqkv, out, u_buf, w_buf, sem = refs[2 * n:]
    core = lax.rem(lax.axis_index('frames'), 2)
    copy = pltpu.make_async_copy(wqkv.at[layer, pl.ds(start, cols)], w_buf, sem)
    copy.start()
    for s in range(OWN):
        u_buf[pl.ds(pl.multiple_of((core * OWN + s) * HALF, HALF), HALF), :] = mine[s // PART][s % PART]
        u_buf[pl.ds(pl.multiple_of(((1 - core) * OWN + s) * HALF, HALF), HALF), :] = theirs[s // PART][s % PART]
    copy.wait()

    def block(j, carry):
        c = pl.ds(pl.multiple_of(j * 256, 256), 256)
        out[:, :, c] = dot_nt(u_buf[...], w_buf[c, :]).astype(BF16).reshape(2 * OWN, HALF, 256)
        return carry

    lax.fori_loop(0, cols // 256, block, 0)


def project_call(layer, mine, theirs, w_tqkv, start, cols):
    rows = 2 * OWN * HALF
    return pl.pallas_call(
        functools.partial(project_kernel, layer=layer, start=start, cols=cols),
        out_shape=jax.ShapeDtypeStruct((2 * OWN, HALF, cols), BF16),
        in_specs=[VM] * (2 * OWN // PART) + [HB],
        out_specs=VM,
        scratch_shapes=[pltpu.VMEM((rows, D), BF16), pltpu.VMEM((cols, D), BF16), pltpu.SemaphoreType.DMA],
        compiler_params=pltpu.CompilerParams(vmem_limit_bytes=VMEM_LIMIT),
        cost_estimate=pl.CostEstimate(flops=2 * rows * D * cols, bytes_accessed=8 << 20, transcendentals=0),
        name='project',
    )(*mine, *theirs, w_tqkv)


def halo_kernel(*refs, layer):
    n = OWN // PART
    q, kv_near, kv_own = refs[:3]
    up_k, up_s, down_k, down_s = (refs[3 + n * i:3 + n * i + n] for i in range(4))
    bias_all, wqkv, o_keep, o_send, u_buf, kv, bias, w_buf, o_buf, sems, halo_sems = refs[3 + 4 * n:]
    pos = lax.axis_index('frames')
    core = lax.rem(pos, 2)
    other = 1 - core
    row = pos // 2
    cw = pltpu.make_async_copy(wqkv.at[layer, pl.ds(D, 2 * D)], w_buf, sems.at[0])
    cw.start()

    def into(src, slot, k):
        return [pltpu.make_async_copy(src[i], u_buf.at[pl.ds(slot + PART * i, PART)], halo_sems.at[k, i]) for i in range(n)]

    up = into(up_k, core * OWN, 0) + into(up_s, other * OWN, 1)
    down = into(down_k, core * OWN, 0) + into(down_s, other * OWN, 1)

    @pl.when(row == 1)
    def _():
        for c in up:
            c.start()

    @pl.when(row == 0)
    def _():
        for c in down:
            c.start()

    c4 = pltpu.make_async_copy(kv_own, kv.at[pl.ds(4 * OWN, 2 * OWN)], sems.at[1])
    c4.start()
    c5 = pltpu.make_async_copy(bias_all.at[layer], bias, sems.at[2])
    c5.start()
    c6 = pltpu.make_async_copy(kv_near, kv.at[pl.ds(0, 2 * OWN)], sems.at[3])
    c6.start()
    for c in [cw] + up:
        c.wait()

    def fill(i, carry):
        s = (i // 8) * 4
        j = i % 8
        c = pl.ds(pl.multiple_of(j * 256, 256), 256)
        a = u_buf[pl.ds(s, 4)].reshape(4 * HALF, D)
        kv[pl.ds(2 * OWN + s, 4), :, c] = dot_nt(a, w_buf[c, :]).astype(BF16).reshape(4, HALF, 256)
        return carry

    lax.fori_loop(0, 16, fill, 0)
    c4.wait()
    c5.wait()
    c6.wait()
    low, high, is_low = half_masks()

    def attend(i, carry):
        tok = pl.ds(pl.multiple_of(i * GRP, GRP), GRP)
        for hp in range(8):
            c = slice(hp * 128, hp * 128 + 128)
            qb = q[:, tok, c].reshape(2 * OWN * GRP, 128)
            key = kv[:, tok, c].reshape(6 * OWN * GRP, 128)
            val = kv[:, tok, D + hp * 128:D + hp * 128 + 128].reshape(6 * OWN * GRP, 128)
            mixed = []
            for e, m in enumerate((low, high)):
                t = dot_nt(key, qb * m) * (0.125 * LOG2E) + bias[2 * hp + e]
                mixed.append(dot_tn(softmax_bf16(t), val))
            o = jnp.where(is_low, mixed[0], mixed[1]).astype(BF16)
            o_buf[:, tok, c] = o.reshape(2 * OWN, GRP, 128)
        return carry

    lax.fori_loop(0, HALF // GRP, attend, 0)
    o_keep[...] = o_buf[pl.ds(core * OWN, OWN)]
    o_send[...] = o_buf[pl.ds(other * OWN, OWN)]


def halo_call(layer, q, kv_near, kv_own, halos, bias, w_tqkv):
    n = 2 * OWN
    return pl.pallas_call(
        functools.partial(halo_kernel, layer=layer),
        out_shape=[jax.ShapeDtypeStruct((OWN, HALF, D), BF16)] * 2,
        in_specs=[VM] + [HB] * (4 + len(halos)),
        out_specs=[VM, VM],
        scratch_shapes=[pltpu.VMEM((n, HALF, D), BF16), pltpu.VMEM((3 * n, HALF, 2 * D), BF16),
                        pltpu.VMEM((16, 3 * n * GRP, n * GRP), F32), pltpu.VMEM((2 * D, D), BF16),
                        pltpu.VMEM((n, HALF, D), BF16), pltpu.SemaphoreType.DMA((4,)),
                        pltpu.SemaphoreType.DMA((2, OWN // PART))],
        compiler_params=pltpu.CompilerParams(vmem_limit_bytes=VMEM_LIMIT),
        cost_estimate=pl.CostEstimate(flops=8 * n * HALF * D * D, bytes_accessed=16 << 20, transcendentals=0),
        name='temporal_halo',
    )(q, kv_near, kv_own, *halos, bias, w_tqkv)


def bias_kernel(lag, out):
    base = 16 * (16 * lax.axis_index('tokens') + 8 * (lax.axis_index('frames') // 2))
    shape = out.shape[2:]
    col = lax.broadcasted_iota(jnp.int32, shape, 0)
    row = lax.broadcasted_iota(jnp.int32, shape, 1)
    gap = jnp.where(col + base >= 256, row + 256 - col, -1)
    layer = pl.program_id(0)

    def head(h, carry):
        acc = jnp.full(shape, -1e30, F32)
        for r in range(16):
            acc = jnp.where(gap == GRP * r, lag[layer, h, r] * LOG2E, acc)
        out[0, h] = acc
        return carry

    lax.fori_loop(0, 16, head, 0)


def bias_call(lag_bias):
    shape = (3, 16, 6 * OWN * GRP, 2 * OWN * GRP)
    return pl.pallas_call(
        bias_kernel,
        grid=(3,),
        out_shape=jax.ShapeDtypeStruct(shape, F32),
        in_specs=[pl.BlockSpec(memory_space=pltpu.SMEM)],
        out_specs=pl.BlockSpec((1,) + shape[1:], lambda i: (i, 0, 0, 0)),
        name='bias_table',
    )(lag_bias)


def solution(mesh):
    nz = mesh.shape['tokens']
    slot_spec = P(('videos', 'frames'), 'tokens', None)
    mod_spec = P(('videos', 'frames'), None, None, None)
    step_spec = P(('videos', 'frames'))
    noise_spec = P('videos', 'tokens', None)
    emit_spec = P('videos', ('tokens', 'frames'), None)
    group = ('tokens', 'frames')
    same = [(z * 4 + f, (z + 1) * 4 + f) for z in range(nz - 1) for f in range(4)]
    cross = [(z * 4 + f, (z + 1) * 4 + (f ^ 1)) for z in range(nz - 1) for f in range(4)]

    back = [(i + 1, i) for i in range(4 * nz - 1)]

    def body(z_loc, mod_loc, step_loc, noise_loc, lag_bias, w_in, w_out, w_sqkv, w_so, w_tqkv, w_to, w_up, w_down):
        zc = lax.axis_index('tokens')
        fc = lax.axis_index('frames')
        layers = w_up.shape[0]
        n_steps = noise_loc.shape[0]
        sq = jnp.transpose(w_sqkv, (0, 2, 3, 4, 1)).reshape(layers, 3 * D, D)
        tq = jnp.transpose(w_tqkv, (0, 2, 3, 4, 1)).reshape(layers, 3 * D, D)
        so = w_so.reshape(layers, D, D)
        to = w_to.reshape(layers, D, D)
        bias = bias_call(lag_bias)

        small = jnp.concatenate([z_loc.reshape(16, 256), noise_loc.reshape(n_steps, 256),
                                 jnp.pad(step_loc, (0, 240))[None]], axis=0)
        small = lax.all_gather(small, group, axis=0).reshape(nz, 4, 17 + n_steps, 256)
        z_all = small[:, :, :16].reshape(nz, 4, 16, 64, 4).transpose(1, 2, 0, 3, 4).reshape(64, TOK * 4)
        noise = small[:, 0, 16:16 + n_steps].reshape(nz, n_steps, 256).transpose(1, 0, 2).reshape(n_steps, TOK * 4)
        first = 16 * zc + 4 * fc
        dt = lax.dynamic_slice(small[0, :, 16 + n_steps, :16].reshape(64), (first,), (4,))
        mod = lax.all_to_all(mod_loc.reshape(4, 4, layers, 6, D), 'frames', 0, 0)
        mod = lax.dynamic_index_in_dim(mod, zc, 0, keepdims=False)
        mods = [[mod[p * PART:(p + 1) * PART, l] for p in range(OWN // PART)] for l in range(layers)]

        def one_step(s, z_own):
            z_cur = z_own.reshape(4 * TOK, 4)
            x = dot(z_cur.astype(BF16), w_in).astype(BF16).astype(F32)
            parts = range(OWN // PART)
            rows = PART * TOK
            xs = [x[p * rows:(p + 1) * rows] for p in parts]
            c_args = None
            for l in range(layers):
                keeps, sends = [], []
                for p in parts:
                    a_args = [mods[l][p], sq, so]
                    ca = () if l == 0 else c_args + [mods[l - 1][p], to, w_up, w_down]
                    if l and p == OWN // PART - 1:
                        xs[p] = dense_call(l - 1, p, True, False, xs[p], ca, ())[0]
                        ca = ()
                    fuse = bool(ca)
                    xs[p], keep, send = dense_call(l - 1 if fuse else l, p, fuse, True, xs[p], ca, a_args)
                    keeps.append(keep)
                    sends.append(send)

                def move(vals, axes, pairs):
                    out = []
                    for p in parts:
                        out.append(lax.ppermute(vals[p], axes, pairs))
                    return out

                near_k = move(keeps, group, same)
                near_s = move(sends, group, cross)
                up_k = move(keeps, 'frames', [(0, 2), (1, 3)])
                up_s = move(sends, 'frames', [(0, 3), (1, 2)])
                swaps = move(sends, 'frames', [(0, 1), (1, 0), (2, 3), (3, 2)])
                down_k = move(near_k, 'frames', [(2, 0), (3, 1)])
                down_s = move(near_s, 'frames', [(2, 0), (3, 1)])
                q = project_call(l, keeps, swaps, tq, 0, D)
                kv_own = project_call(l, keeps, swaps, tq, D, 2 * D)
                kv_near = project_call(l, near_k, near_s, tq, D, 2 * D)
                o_keep, o_send = halo_call(l, q, kv_near, kv_own, up_k + up_s + down_k + down_s, bias, tq)
                o_recv = lax.ppermute(o_send, 'frames', [(0, 1), (1, 0), (2, 3), (3, 2)])
                c_args = [o_keep, o_recv]
            xs = [dense_call(layers - 1, p, True, False, xs[p], c_args + [mods[layers - 1][p], to, w_up, w_down], ())[0]
                  for p in parts]
            x = jnp.concatenate(xs, axis=0)
            vel = dot(norm_rows(x).astype(BF16), w_out)
            z_new = (z_cur + jnp.repeat(dt, TOK)[:, None] * vel).reshape(4, TOK * 4)
            after = lax.ppermute(z_new[0], group, back)
            after = jnp.where(first == 16 * nz - 4, noise[s], after)
            return jnp.concatenate([z_new[1:], after[None]], axis=0), z_new[:1]

        z_own = lax.dynamic_slice(z_all, (first, 0), (4, TOK * 4))
        heads = []
        for s in range(n_steps):
            z_own, head = one_step(s, z_own)
            heads.append(head)
        last = lax.all_gather(jnp.concatenate([z_own] + heads, axis=0), group, axis=0)
        emits = lax.dynamic_slice(last[0, 4:].reshape(n_steps, TOK, 4), (0, 64 * zc + 16 * fc, 0), (n_steps, 16, 4))
        z_out = lax.dynamic_slice(last[:, :4].reshape(16 * nz, TOK, 4), (16 * fc, 64 * zc, 0), (16, 64, 4))
        return emits, z_out

    return jax.shard_map(body, mesh=mesh, in_specs=(slot_spec, mod_spec, step_spec, noise_spec) + (P(),) * 9,
                         out_specs=(emit_spec, slot_spec), check_vma=False)
```

```python
import functools

import jax
import jax.numpy as jnp
from jax import lax
from jax.experimental import pallas as pl
from jax.experimental.pallas import tpu as pltpu
from jax.sharding import PartitionSpec as P


F32 = jnp.float32
BF16 = jnp.bfloat16
LOG2E = 1.4426950408889634
D = 1024
HID = 4096
TOK = 256
HALF = 128
OWN = 4
GRP = 16
VMEM_LIMIT = 66_000_000
NT = (((1,), (1,)), ((), ()))
TN = (((0,), (0,)), ((), ()))
PART = 2
COLS = 512


def dot(a, b):
    return jnp.dot(a, b, preferred_element_type=F32)


def dot_nt(a, b):
    return lax.dot_general(a, b, NT, preferred_element_type=F32)


def norm_rows(xb):
    mean = jnp.mean(xb, axis=-1, keepdims=True)
    cen = xb - mean
    var = jnp.mean(cen * cen, axis=-1, keepdims=True)
    return cen * lax.rsqrt(var + 1e-6)


def norm_mod(src, src_row, dst, dst_row, shift, scale, rows, blk=128):
    gain = 1.0 + scale

    def body(i, carry):
        rs = pl.multiple_of(src_row + i * blk, blk)
        rd = pl.multiple_of(dst_row + i * blk, blk)
        dst[pl.ds(rd, blk), :] = (norm_rows(src[pl.ds(rs, blk), :]) * gain + shift).astype(BF16)
        return carry

    lax.fori_loop(0, rows // blk, body, 0)


def gelu(v):
    return v * (0.5 + 0.5 * jnp.tanh(v * (0.7978845608028654 + (0.7978845608028654 * 0.044715) * (v * v))))


def dot_tn(a, b):
    return lax.dot_general(a, b, TN, preferred_element_type=F32)


def softmax_bf16(t):
    top = jnp.max(t, axis=0, keepdims=True)
    e = jnp.exp2(t - top)
    return (e * (1.0 / jnp.sum(e, axis=0, keepdims=True))).astype(BF16)


def half_masks():
    lane = lax.broadcasted_iota(jnp.int32, (1, 128), 1)
    low = (lane < 64).astype(F32)
    return low.astype(BF16), (1.0 - low).astype(BF16), lane < 64


def dense_kernel(*refs, do_c, do_a, ns, layer, part):
    it = iter(refs)
    x_in = next(it)
    if do_c:
        o_keep, o_recv, mod_c, wto, wup, wdn = (next(it) for _ in range(6))
    if do_a:
        mod_a, wsqkv, wso = (next(it) for _ in range(3))
    x = next(it)
    if do_a:
        u_keep, u_send = next(it), next(it)
    u_buf, o_buf = next(it), next(it)
    if do_c:
        vto, vup, vdn, h_buf = (next(it) for _ in range(4))
    if do_a:
        vsqkv, vso, qkv_buf = (next(it) for _ in range(3))
    sems = next(it)

    rows = ns * TOK
    core = lax.rem(lax.axis_index('frames'), 2)
    copies = []
    if do_c:
        copies += [pltpu.make_async_copy(wto.at[layer], vto, sems.at[0]),
                   pltpu.make_async_copy(wup.at[layer], vup, sems.at[1]),
                   pltpu.make_async_copy(wdn.at[layer], vdn, sems.at[2])]
    nxt = layer + 1 if do_c else layer
    if do_a:
        copies += [pltpu.make_async_copy(wsqkv.at[nxt], vsqkv, sems.at[3]),
                   pltpu.make_async_copy(wso.at[nxt], vso, sems.at[4])]
    state = {'next': 0}

    def start_more():
        if state['next'] < len(copies):
            copies[state['next']].start()
            state['next'] += 1

    def arrive(k):
        copies[k].wait()
        start_more()

    start_more()
    start_more()
    k = 0
    if do_c:
        for s in range(ns):
            o_buf[pl.ds(pl.multiple_of(s * TOK + core * HALF, HALF), HALF), :] = o_keep[part * ns + s]
            o_buf[pl.ds(pl.multiple_of(s * TOK + (1 - core) * HALF, HALF), HALF), :] = o_recv[part * ns + s]
        arrive(0)

        def proj(j, carry):
            c = pl.ds(pl.multiple_of(j * COLS, COLS), COLS)
            x[:, c] = x_in[:, c] + dot(o_buf[...], vto[:, c])
            return carry

        lax.fori_loop(0, D // COLS, proj, 0)
        for s in range(ns):
            norm_mod(x, s * TOK, u_buf, s * TOK, mod_c[s, 4:5, :], mod_c[s, 5:6, :], TOK)
        arrive(1)
        hrows = min(rows, 512)
        for b in range(rows // hrows):
            rb = pl.ds(b * hrows, hrows)

            def up(j, carry):
                c = pl.ds(pl.multiple_of(j * COLS, COLS), COLS)
                h_buf[:, c] = gelu(dot(u_buf[rb, :], vup[:, c])).astype(BF16)
                return carry

            lax.fori_loop(0, HID // COLS, up, 0)
            if b == 0:
                arrive(2)

            def down(j, carry):
                c = pl.ds(pl.multiple_of(j * COLS, COLS), COLS)
                x[rb, c] = x[rb, c] + dot(h_buf[...], vdn[:, c])
                return carry

            lax.fori_loop(0, D // COLS, down, 0)
        k = 3
    else:
        x[...] = x_in[...]
    if do_a:
        for s in range(ns):
            norm_mod(x, s * TOK, u_buf, s * TOK, mod_a[s, 0:1, :], mod_a[s, 1:2, :], TOK)
        arrive(k)

        def qkv(j, carry):
            c = pl.ds(pl.multiple_of(j * COLS, COLS), COLS)
            qkv_buf[:, c] = dot_nt(u_buf[...], vsqkv[c, :]).astype(BF16)
            return carry

        lax.fori_loop(0, 3 * D // COLS, qkv, 0)
        low, high, is_low = half_masks()

        def attend(i, carry):
            r = pl.ds(pl.multiple_of((i // 2) * TOK, TOK), TOK)
            for h in range(4):
                c = (i % 2) * 512 + h * 128
                q = qkv_buf[r, pl.ds(pl.multiple_of(c, 128), 128)]
                key = qkv_buf[r, pl.ds(pl.multiple_of(D + c, 128), 128)]
                val = qkv_buf[r, pl.ds(pl.multiple_of(2 * D + c, 128), 128)]
                both = jnp.concatenate([q * low, q * high], axis=0)
                mixed = dot_tn(softmax_bf16(dot_nt(key, both) * (0.125 * LOG2E)), val)
                o_buf[r, pl.ds(pl.multiple_of(c, 128), 128)] = jnp.where(is_low, mixed[:TOK], mixed[TOK:]).astype(BF16)
            return carry

        lax.fori_loop(0, ns * 2, attend, 0)
        arrive(k + 1)

        def proj_s(j, carry):
            c = pl.ds(pl.multiple_of(j * COLS, COLS), COLS)
            x[:, c] = x[:, c] + dot(o_buf[...], vso[:, c])
            return carry

        lax.fori_loop(0, D // COLS, proj_s, 0)
        for s in range(ns):
            norm_mod(x, s * TOK + core * HALF, u_keep.at[s], 0, mod_a[s, 2:3, :], mod_a[s, 3:4, :], HALF)
            norm_mod(x, s * TOK + (1 - core) * HALF, u_send.at[s], 0, mod_a[s, 2:3, :], mod_a[s, 3:4, :], HALF)


VM = pl.BlockSpec(memory_space=pltpu.VMEM)
HB = pl.BlockSpec(memory_space=pl.ANY)


def dense_call(layer, part, do_c, do_a, x, c_args, a_args):
    rows = x.shape[0]
    ns = rows // TOK
    args, specs = [x], [VM]
    if do_c:
        args += c_args
        specs += [VM, VM, VM, HB, HB, HB]
    if do_a:
        args += a_args
        specs += [VM, HB, HB]
    outs = [jax.ShapeDtypeStruct((rows, D), F32)]
    if do_a:
        outs += [jax.ShapeDtypeStruct((ns, HALF, D), BF16)] * 2
    scratch = [pltpu.VMEM((rows, D), BF16), pltpu.VMEM((rows, D), BF16)]
    if do_c:
        scratch += [pltpu.VMEM((D, D), BF16), pltpu.VMEM((D, HID), BF16), pltpu.VMEM((HID, D), BF16),
                    pltpu.VMEM((min(rows, 512), HID), BF16)]
    if do_a:
        scratch += [pltpu.VMEM((3 * D, D), BF16), pltpu.VMEM((D, D), BF16), pltpu.VMEM((rows, 3 * D), BF16)]
    scratch.append(pltpu.SemaphoreType.DMA((5,)))
    flops = 2 * rows * D * ((D + 2 * HID) * do_c + 4 * D * do_a)
    return pl.pallas_call(
        functools.partial(dense_kernel, do_c=do_c, do_a=do_a, ns=ns, layer=layer, part=part),
        out_shape=outs,
        in_specs=specs,
        out_specs=[VM] * len(outs),
        scratch_shapes=scratch,
        compiler_params=pltpu.CompilerParams(vmem_limit_bytes=VMEM_LIMIT),
        cost_estimate=pl.CostEstimate(flops=flops, bytes_accessed=rows * D * 8, transcendentals=0),
        name='dense',
    )(*args)


def project_kernel(*refs):
    n = OWN // PART
    mine, theirs = refs[:n], refs[n:2 * n]
    w_blk, out, u_buf = refs[2 * n:]
    core = lax.rem(lax.axis_index('frames'), 2)

    @pl.when(pl.program_id(0) == 0)
    def _():
        for s in range(OWN):
            u_buf[pl.ds(pl.multiple_of((core * OWN + s) * HALF, HALF), HALF), :] = mine[s // PART][s % PART]
            u_buf[pl.ds(pl.multiple_of(((1 - core) * OWN + s) * HALF, HALF), HALF), :] = theirs[s // PART][s % PART]

    out[...] = dot_nt(u_buf[...], w_blk[...]).astype(BF16).reshape(2 * OWN, HALF, out.shape[-1])


def project_call(layer, mine, theirs, w_tqkv, start, cols, blk=512):
    rows = 2 * OWN * HALF
    return pl.pallas_call(
        project_kernel,
        grid=(cols // blk,),
        out_shape=jax.ShapeDtypeStruct((2 * OWN, HALF, cols), BF16),
        in_specs=[pl.BlockSpec((PART, HALF, D), lambda j: (0, 0, 0))] * (2 * OWN // PART)
        + [pl.BlockSpec((None, blk, D), lambda j: (layer, start // blk + j, 0))],
        out_specs=pl.BlockSpec((2 * OWN, HALF, blk), lambda j: (0, 0, j)),
        scratch_shapes=[pltpu.VMEM((rows, D), BF16)],
        compiler_params=pltpu.CompilerParams(vmem_limit_bytes=VMEM_LIMIT),
        cost_estimate=pl.CostEstimate(flops=2 * rows * D * cols, bytes_accessed=8 << 20, transcendentals=0),
        name='project',
    )(*mine, *theirs, w_tqkv)


def halo_kernel(*refs, layer):
    n = OWN // PART
    q, kv_near, kv_own = refs[:3]
    up_k, up_s, down_k, down_s = (refs[3 + n * i:3 + n * i + n] for i in range(4))
    bias_all, wqkv, o_keep, o_send, u_buf, kv, bias, w_buf, o_buf, sems, halo_sems = refs[3 + 4 * n:]
    pos = lax.axis_index('frames')
    core = lax.rem(pos, 2)
    other = 1 - core
    row = pos // 2
    cw = pltpu.make_async_copy(wqkv.at[layer, pl.ds(D, 2 * D)], w_buf, sems.at[0])
    cw.start()

    def into(src, slot, k):
        return [pltpu.make_async_copy(src[i], u_buf.at[pl.ds(slot + PART * i, PART)], halo_sems.at[k, i]) for i in range(n)]

    up = into(up_k, core * OWN, 0) + into(up_s, other * OWN, 1)
    down = into(down_k, core * OWN, 0) + into(down_s, other * OWN, 1)

    @pl.when(row == 1)
    def _():
        for c in up:
            c.start()

    @pl.when(row == 0)
    def _():
        for c in down:
            c.start()

    c4 = pltpu.make_async_copy(kv_own, kv.at[pl.ds(4 * OWN, 2 * OWN)], sems.at[1])
    c4.start()
    c5 = pltpu.make_async_copy(bias_all.at[layer], bias, sems.at[2])
    c5.start()
    c6 = pltpu.make_async_copy(kv_near, kv.at[pl.ds(0, 2 * OWN)], sems.at[3])
    c6.start()
    for c in [cw] + up:
        c.wait()

    def fill(i, carry):
        s = (i // 4) * 4
        j = i % 4
        c = pl.ds(pl.multiple_of(j * COLS, COLS), COLS)
        a = u_buf[pl.ds(s, 4)].reshape(4 * HALF, D)
        kv[pl.ds(2 * OWN + s, 4), :, c] = dot_nt(a, w_buf[c, :]).astype(BF16).reshape(4, HALF, COLS)
        return carry

    lax.fori_loop(0, 8, fill, 0)
    c4.wait()
    c5.wait()
    c6.wait()
    low, high, is_low = half_masks()

    def attend(i, carry):
        tok = pl.ds(pl.multiple_of(i * GRP, GRP), GRP)
        for hp in range(8):
            c = slice(hp * 128, hp * 128 + 128)
            qb = q[:, tok, c].reshape(2 * OWN * GRP, 128)
            key = kv[:, tok, c].reshape(6 * OWN * GRP, 128)
            val = kv[:, tok, D + hp * 128:D + hp * 128 + 128].reshape(6 * OWN * GRP, 128)
            mixed = []
            for e, m in enumerate((low, high)):
                t = dot_nt(key, qb * m) * (0.125 * LOG2E) + bias[2 * hp + e]
                mixed.append(dot_tn(softmax_bf16(t), val))
            o = jnp.where(is_low, mixed[0], mixed[1]).astype(BF16)
            o_buf[:, tok, c] = o.reshape(2 * OWN, GRP, 128)
        return carry

    lax.fori_loop(0, HALF // GRP, attend, 0)
    o_keep[...] = o_buf[pl.ds(core * OWN, OWN)]
    o_send[...] = o_buf[pl.ds(other * OWN, OWN)]


def halo_call(layer, q, kv_near, kv_own, halos, bias, w_tqkv):
    n = 2 * OWN
    return pl.pallas_call(
        functools.partial(halo_kernel, layer=layer),
        out_shape=[jax.ShapeDtypeStruct((OWN, HALF, D), BF16)] * 2,
        in_specs=[VM] + [HB] * (4 + len(halos)),
        out_specs=[VM, VM],
        scratch_shapes=[pltpu.VMEM((n, HALF, D), BF16), pltpu.VMEM((3 * n, HALF, 2 * D), BF16),
                        pltpu.VMEM((16, 3 * n * GRP, n * GRP), F32), pltpu.VMEM((2 * D, D), BF16),
                        pltpu.VMEM((n, HALF, D), BF16), pltpu.SemaphoreType.DMA((4,)),
                        pltpu.SemaphoreType.DMA((2, OWN // PART))],
        compiler_params=pltpu.CompilerParams(vmem_limit_bytes=VMEM_LIMIT),
        cost_estimate=pl.CostEstimate(flops=8 * n * HALF * D * D, bytes_accessed=16 << 20, transcendentals=0),
        name='temporal_halo',
    )(q, kv_near, kv_own, *halos, bias, w_tqkv)


def bias_kernel(lag, out):
    base = 16 * (16 * lax.axis_index('tokens') + 8 * (lax.axis_index('frames') // 2))
    shape = out.shape[2:]
    col = lax.broadcasted_iota(jnp.int32, shape, 0)
    row = lax.broadcasted_iota(jnp.int32, shape, 1)
    gap = jnp.where(col + base >= 256, row + 256 - col, -1)
    layer = pl.program_id(0)

    def head(h, carry):
        acc = jnp.full(shape, -1e30, F32)
        for r in range(16):
            acc = jnp.where(gap == GRP * r, lag[layer, h, r] * LOG2E, acc)
        out[0, h] = acc
        return carry

    lax.fori_loop(0, 16, head, 0)


def bias_call(lag_bias):
    shape = (3, 16, 6 * OWN * GRP, 2 * OWN * GRP)
    return pl.pallas_call(
        bias_kernel,
        grid=(3,),
        out_shape=jax.ShapeDtypeStruct(shape, F32),
        in_specs=[pl.BlockSpec(memory_space=pltpu.SMEM)],
        out_specs=pl.BlockSpec((1,) + shape[1:], lambda i: (i, 0, 0, 0)),
        name='bias_table',
    )(lag_bias)


def solution(mesh):
    nz = mesh.shape['tokens']
    slot_spec = P(('videos', 'frames'), 'tokens', None)
    mod_spec = P(('videos', 'frames'), None, None, None)
    step_spec = P(('videos', 'frames'))
    noise_spec = P('videos', 'tokens', None)
    emit_spec = P('videos', ('tokens', 'frames'), None)
    group = ('tokens', 'frames')
    same = [(z * 4 + f, (z + 1) * 4 + f) for z in range(nz - 1) for f in range(4)]
    cross = [(z * 4 + f, (z + 1) * 4 + (f ^ 1)) for z in range(nz - 1) for f in range(4)]

    back = [(i + 1, i) for i in range(4 * nz - 1)]

    def body(z_loc, mod_loc, step_loc, noise_loc, lag_bias, w_in, w_out, w_sqkv, w_so, w_tqkv, w_to, w_up, w_down):
        zc = lax.axis_index('tokens')
        fc = lax.axis_index('frames')
        layers = w_up.shape[0]
        n_steps = noise_loc.shape[0]
        sq = jnp.transpose(w_sqkv, (0, 2, 3, 4, 1)).reshape(layers, 3 * D, D)
        tq = jnp.transpose(w_tqkv, (0, 2, 3, 4, 1)).reshape(layers, 3 * D, D)
        so = w_so.reshape(layers, D, D)
        to = w_to.reshape(layers, D, D)
        bias = bias_call(lag_bias)

        small = jnp.concatenate([z_loc.reshape(16, 256), noise_loc.reshape(n_steps, 256),
                                 jnp.pad(step_loc, (0, 240))[None]], axis=0)
        small = lax.all_gather(small, group, axis=0).reshape(nz, 4, 17 + n_steps, 256)
        z_all = small[:, :, :16].reshape(nz, 4, 16, 64, 4).transpose(1, 2, 0, 3, 4).reshape(64, TOK * 4)
        noise = small[:, 0, 16:16 + n_steps].reshape(nz, n_steps, 256).transpose(1, 0, 2).reshape(n_steps, TOK * 4)
        first = 16 * zc + 4 * fc
        dt = lax.dynamic_slice(small[0, :, 16 + n_steps, :16].reshape(64), (first,), (4,))
        mod = lax.all_to_all(mod_loc.reshape(4, 4, layers, 6, D), 'frames', 0, 0)
        mod = lax.dynamic_index_in_dim(mod, zc, 0, keepdims=False)
        mods = [[mod[p * PART:(p + 1) * PART, l] for p in range(OWN // PART)] for l in range(layers)]

        def one_step(s, z_own):
            z_cur = z_own.reshape(4 * TOK, 4)
            x = dot(z_cur.astype(BF16), w_in).astype(BF16).astype(F32)
            parts = range(OWN // PART)
            rows = PART * TOK
            xs = [x[p * rows:(p + 1) * rows] for p in parts]
            c_args = None
            for l in range(layers):
                keeps, sends = [], []
                for p in parts:
                    a_args = [mods[l][p], sq, so]
                    ca = () if l == 0 else c_args + [mods[l - 1][p], to, w_up, w_down]
                    if l and p == OWN // PART - 1:
                        xs[p] = dense_call(l - 1, p, True, False, xs[p], ca, ())[0]
                        ca = ()
                    fuse = bool(ca)
                    xs[p], keep, send = dense_call(l - 1 if fuse else l, p, fuse, True, xs[p], ca, a_args)
                    keeps.append(keep)
                    sends.append(send)

                def move(vals, axes, pairs):
                    out = []
                    for p in parts:
                        out.append(lax.ppermute(vals[p], axes, pairs))
                    return out

                near_k = move(keeps, group, same)
                near_s = move(sends, group, cross)
                up_k = move(keeps, 'frames', [(0, 2), (1, 3)])
                up_s = move(sends, 'frames', [(0, 3), (1, 2)])
                swaps = move(sends, 'frames', [(0, 1), (1, 0), (2, 3), (3, 2)])
                down_k = move(near_k, 'frames', [(2, 0), (3, 1)])
                down_s = move(near_s, 'frames', [(2, 0), (3, 1)])
                q = project_call(l, keeps, swaps, tq, 0, D)
                kv_own = project_call(l, keeps, swaps, tq, D, 2 * D)
                kv_near = project_call(l, near_k, near_s, tq, D, 2 * D)
                o_keep, o_send = halo_call(l, q, kv_near, kv_own, up_k + up_s + down_k + down_s, bias, tq)
                o_recv = lax.ppermute(o_send, 'frames', [(0, 1), (1, 0), (2, 3), (3, 2)])
                c_args = [o_keep, o_recv]
            xs = [dense_call(layers - 1, p, True, False, xs[p], c_args + [mods[layers - 1][p], to, w_up, w_down], ())[0]
                  for p in parts]
            x = jnp.concatenate(xs, axis=0)
            vel = dot(norm_rows(x).astype(BF16), w_out)
            z_new = (z_cur + jnp.repeat(dt, TOK)[:, None] * vel).reshape(4, TOK * 4)
            after = lax.ppermute(z_new[0], group, back)
            after = jnp.where(first == 16 * nz - 4, noise[s], after)
            return jnp.concatenate([z_new[1:], after[None]], axis=0), z_new[:1]

        z_own = lax.dynamic_slice(z_all, (first, 0), (4, TOK * 4))
        heads = []
        for s in range(n_steps):
            z_own, head = one_step(s, z_own)
            heads.append(head)
        last = lax.all_gather(jnp.concatenate([z_own] + heads, axis=0), group, axis=0)
        emits = lax.dynamic_slice(last[0, 4:].reshape(n_steps, TOK, 4), (0, 64 * zc + 16 * fc, 0), (n_steps, 16, 4))
        z_out = lax.dynamic_slice(last[:, :4].reshape(16 * nz, TOK, 4), (16 * fc, 64 * zc, 0), (16, 64, 4))
        return emits, z_out

    return jax.shard_map(body, mesh=mesh, in_specs=(slot_spec, mod_spec, step_spec, noise_spec) + (P(),) * 9,
                         out_specs=(emit_spec, slot_spec), check_vma=False)
```
